32 devices in a mesh: fsdp: 8 (over z, x), tp: 4 (over y, core).
Axes of the slice: x: 2, y: 2, z: 4, core: 2. Of those that a mesh axis runs over, the one named last changes fastest.
Arguments:
- hidden_in: bfloat16 [3, 2048, 2048], P(None, ('fsdp', 'tp')), may hold values from -6 to 6
- cotangent: float32 [3, 2048, 2048], P(None, ('fsdp', 'tp')), may hold values from -6 to 6
- gain_attn: float32 [2048], P(('fsdp', 'tp')), may hold values from 0.1 to 1.9
- w_query: bfloat16 [2048, 2048], P('fsdp', 'tp'), may hold values from -0.125 to 0.125
- w_key: bfloat16 [2048, 256], P('fsdp', 'tp'), may hold values from -0.125 to 0.125
- w_value: bfloat16 [2048, 256], P('fsdp', 'tp'), may hold values from -0.125 to 0.125
- w_out: bfloat16 [2048, 2048], P('tp', 'fsdp'), may hold values from -3 to 3
- gain_mlp: float32 [2048], P(('fsdp', 'tp')), may hold values from 0.1 to 1.9
- w_gate: bfloat16 [2048, 5632], P('fsdp', 'tp'), may hold values from -0.125 to 0.125
- w_up: bfloat16 [2048, 5632], P('fsdp', 'tp'), may hold values from -0.125 to 0.125
- w_down: bfloat16 [5632, 2048], P('tp', 'fsdp'), may hold values from -0.078125 to 0.078125
- prefix: int32 [3], replicated, may hold values from 204 to 1024
- block_order: int32 [3, 8], replicated, may hold values from 0 to 7, each once within a row
Outputs:
- layer_out: float32 [3, 2048, 2048], P(None, ('fsdp', 'tp'))
- grad_in: float32 [3, 2048, 2048], P(None, ('fsdp', 'tp'))
- grad_attn: float32 [2048], P(('fsdp', 'tp'))
- grad_query: float32 [2048, 2048], P('fsdp', 'tp')
- grad_key: float32 [2048, 256], P('fsdp', 'tp')
- grad_value: float32 [2048, 256], P('fsdp', 'tp')
- grad_out: float32 [2048, 2048], P('tp', 'fsdp')
- grad_mlp: float32 [2048], P(('fsdp', 'tp'))
- grad_gate: float32 [2048, 5632], P('fsdp', 'tp')
- grad_up: float32 [2048, 5632], P('fsdp', 'tp')
- grad_down: float32 [5632, 2048], P('tp', 'fsdp')
The draws below stay inside these ranges and needn't reach their ends.
Inputs may be any that keep to these rules, and one draw needn't show every extreme that they name: `prefix`: the number of leading positions of each sequence that attend to one another in both directions. `block_order`: row s names, for each stored block of 256 rows of sequence s in order, which block of positions it holds; each block once.
All inputs are finite; a program needn't handle non-finite values.
Results may differ from the reference program's by a relative error of at most 0.02.
Values may be sent and summed in bfloat16 or wider, within the bound.
A program may use at most 832 MiB of HBM per device.

```python
import math
import jax
import jax.numpy as jnp
from jax import lax

D = 2048
H = 32
KV = 4
HD = 64
FF = 5632
SEQS = 3
BLOCK = 256
SEQ_LEN = 2048
N_FSDP = 8


def levels(rng, extent, split, least, high):
    factor_of, own = 1.0, jax.random.fold_in(rng, 6)
    for position, shards_of in split:
        steps = jnp.exp(jax.random.uniform(jax.random.fold_in(own, position), (shards_of,), jnp.float32, least / len(split), high / len(split)))
        factor_of = factor_of * jnp.repeat(steps, extent[position] // shards_of).reshape([-1 if axis == position else 1 for axis in range(len(extent))])
    return factor_of


def scatter_about(stream_key, shape, width, bound, cuts=(), kind=jnp.bfloat16):
    entries = width * jax.random.normal(stream_key, shape, jnp.float32)
    if cuts:
        entries = entries * levels(stream_key, shape, cuts, -0.22, 0.18)
    return jnp.clip(entries, -bound, bound).astype(kind)


def setup_inputs(seed: int = 0) -> dict:
    key_of = jax.random.split(jax.random.key(seed), 14)
    hidden_in = scatter_about(key_of[0], (SEQS, SEQ_LEN, D), 1.0, 6.0, ((1, 32),))
    cotangent = scatter_about(key_of[1], (SEQS, SEQ_LEN, D), 1.0, 6.0, ((1, 32),), jnp.float32)
    gain_attn = jnp.clip(1.0 + 0.18 * jax.random.normal(key_of[2], (D,), jnp.float32), 0.1, 1.9)
    w_query = scatter_about(key_of[3], (D, H * HD), D ** -0.5, 0.125, ((0, 8), (1, 4)))
    w_key = scatter_about(key_of[4], (D, KV * HD), D ** -0.5, 0.125, ((0, 8), (1, 4)))
    w_value = scatter_about(key_of[5], (D, KV * HD), D ** -0.5, 0.125, ((0, 8), (1, 4)))
    w_out = scatter_about(key_of[6], (H * HD, D), (max(1, 4 * H * HD // SEQ_LEN)) ** -0.5, 3.0, ((0, 4), (1, 8)))
    gain_mlp = jnp.clip(1.0 + 0.18 * jax.random.normal(key_of[7], (D,), jnp.float32), 0.1, 1.9)
    w_gate = scatter_about(key_of[8], (D, FF), D ** -0.5, 0.125, ((0, 8), (1, 4)))
    w_up = scatter_about(key_of[9], (D, FF), D ** -0.5, 0.125, ((0, 8), (1, 4)))
    w_down = scatter_about(key_of[10], (FF, D), FF ** -0.5, 0.078125, ((0, 4), (1, 8)))
    prefix = jax.random.randint(key_of[11], (SEQS,), SEQ_LEN // 10, SEQ_LEN // 2 + 1).astype(jnp.int32)
    block_order = jax.vmap(lambda own: jax.random.permutation(own, N_FSDP))(jax.random.split(key_of[12], SEQS)).reshape((SEQS, N_FSDP)).astype(jnp.int32)
    return dict(hidden_in=hidden_in, cotangent=cotangent, gain_attn=gain_attn, w_query=w_query, w_key=w_key, w_value=w_value, w_out=w_out, gain_mlp=gain_mlp, w_gate=w_gate, w_up=w_up, w_down=w_down, prefix=prefix, block_order=block_order)


EPS = 1e-05
THETA = 10000.0
NEG = -1000000000.0

@jax.custom_vjp
def low(v):
    return lax.optimization_barrier(v.astype(jnp.bfloat16)).astype(jnp.float32)

@jax.custom_vjp
def low_back(v):
    return v

def low_keep(v):
    return (low(v), None)

def low_pass(kept, grad):
    return (grad,)

def back_keep(v):
    return (v, None)

def back_low(kept, grad):
    return (low(grad),)
low.defvjp(low_keep, low_pass)
low_back.defvjp(back_keep, back_low)

def matmul_high(operand, partner):
    return jnp.dot(operand, partner, precision=lax.Precision.HIGHEST, preferred_element_type=jnp.float32)

def rms_norm(values, gain_vec):
    return values * lax.rsqrt(lax.optimization_barrier(jnp.mean(values * values, axis=-1, keepdims=True)) + EPS) * gain_vec

def rope_tables(positions, head_width):
    halfway = head_width // 2
    frequency = THETA ** (-(jnp.arange(halfway, dtype=jnp.float32) * 2.0 / head_width))
    angles = positions.astype(jnp.float32)[..., None] * frequency
    cos_half = jnp.cos(angles)
    sin_half = jnp.sin(angles)
    return (jnp.concatenate([cos_half, cos_half], -1)[..., None, :], jnp.concatenate([sin_half, sin_half], -1)[..., None, :])

def rotate(values, cos_part, sin_part):
    halfway = values.shape[-1] // 2
    turned = jnp.concatenate([-values[..., halfway:], values[..., :halfway]], -1)
    return values * cos_part + turned * sin_part

def sequence_layer(params, inputs):
    gain_attn, w_query, w_key, w_value, w_out, gain_mlp, w_gate, w_up, w_down = params
    tokens, positions, prefix_len = inputs
    length = tokens.shape[0]
    group_size = H // KV
    h_first = low(rms_norm(tokens, gain_attn))
    cos_part, sin_part = rope_tables(positions, HD)
    queries = low(rotate(low_back(matmul_high(h_first, w_query)).reshape(length, H, HD), cos_part, sin_part))
    keys = low(rotate(low_back(matmul_high(h_first, w_key)).reshape(length, KV, HD), cos_part, sin_part))
    values = low(low_back(matmul_high(h_first, w_value))).reshape(length, KV, HD)
    block_rows = math.gcd(length, 512)
    grouped = queries.reshape(length // block_rows, block_rows, KV, group_size, HD)
    query_blocks = positions.reshape(length // block_rows, block_rows)

    def attend(pieces):
        query_block, query_pos = pieces
        scores = low_back(jnp.einsum('qcgd,kcd->cgqk', query_block, keys, precision=lax.Precision.HIGHEST) * HD ** (-0.5))
        allowed = (positions[None, :] <= query_pos[:, None]) | (positions[None, :] < prefix_len)
        scores = jnp.where(allowed, scores, NEG)
        shifted = jnp.exp(scores - lax.optimization_barrier(jnp.max(scores, axis=-1, keepdims=True)))
        probs = shifted / lax.optimization_barrier(jnp.sum(shifted, axis=-1, keepdims=True))
        return jnp.einsum('cgqk,kcd->qcgd', low(probs), values, precision=lax.Precision.HIGHEST)
    attended = lax.map(jax.checkpoint(attend), (grouped, query_blocks)).reshape(length, H * HD)
    attended = low_back(low(attended))
    middle = tokens + low_back(matmul_high(attended, w_out))
    h_second = low(rms_norm(middle, gain_mlp))
    gate_act = low_back(matmul_high(h_second, w_gate))
    up_act = low_back(matmul_high(h_second, w_up))
    hidden = low(gate_act * jax.nn.sigmoid(gate_act) * up_act)
    return middle + low_back(matmul_high(hidden, w_down))

def reference(hidden_in, cotangent, gain_attn, w_query, w_key, w_value, w_out, gain_mlp, w_gate, w_up, w_down, prefix, block_order):
    offsets = jnp.arange(SEQ_LEN, dtype=jnp.int32)
    positions = (block_order[:, offsets // BLOCK] * BLOCK + offsets % BLOCK).astype(jnp.int32)
    params = jax.tree.map(lambda weight: weight.astype(jnp.float32), (gain_attn, w_query, w_key, w_value, w_out, gain_mlp, w_gate, w_up, w_down))

    def forward(tokens, weights):
        return lax.map(lambda inputs: sequence_layer(weights, inputs), (tokens, positions, prefix))
    layer_out, pullback = jax.vjp(forward, hidden_in.astype(jnp.float32), params)
    grad_in, grads = pullback(cotangent.astype(jnp.float32))
    return (layer_out, grad_in, grads[0], grads[1], grads[2], grads[3], grads[4], grads[5], grads[6], grads[7], grads[8])
```

```python
import functools

import jax
import jax.numpy as jnp
from jax import lax
from jax.experimental import pallas as pl
from jax.experimental.pallas import tpu as pltpu
from jax.sharding import PartitionSpec as P

HD = 64
EPS = 1e-05
THETA = 10000.0
NEG = -1000000000.0
F32 = jnp.float32
BF16 = jnp.bfloat16


def inverse_rms(values):
    return lax.rsqrt(jnp.mean(values * values, axis=-1, keepdims=True) + EPS)


def norm_back(upstream, values, gain_vec, inv_rms):
    weighted = upstream * gain_vec
    inner_mean = jnp.mean(weighted * values, axis=-1, keepdims=True)
    return (
        inv_rms * weighted - values * (inv_rms * inv_rms * inv_rms) * inner_mean,
        jnp.sum(upstream * values * inv_rms, axis=(0, 1)),
    )


def dot(a, b, ca, cb):
    return lax.dot_general(a, b, (((ca,), (cb,)), ((), ())), preferred_element_type=F32)


def swap_b(v):
    n = lax.axis_size("fsdp")
    return lax.ppermute(v, "fsdp", [(i, i ^ 1) for i in range(n)])


def a_groups():
    n = lax.axis_size("fsdp")
    return [[b + 2 * a for a in range(n // 2)] for b in range(2)]


def gather_halves(shard):
    own = lax.all_gather(shard, "fsdp", axis=0, tiled=True, axis_index_groups=a_groups())
    return own, swap_b(own)


def scatter_halves(send, keep_fn):
    other = swap_b(send.astype(BF16))
    total = (keep_fn() + other.astype(F32)).astype(BF16)
    return lax.psum_scatter(
        total, "fsdp", scatter_dimension=0, tiled=True, axis_index_groups=a_groups()
    )


def swap_tp(v, bit):
    n = lax.axis_size("tp")
    return lax.ppermute(v, "tp", [(i, i ^ bit) for i in range(n)])


def spread_rows(v):
    pair = jnp.concatenate([v, swap_tp(v, 2)], axis=1)
    return jnp.concatenate([pair, swap_tp(pair, 1)], axis=1)


def collect_rows(halves):
    out = []
    for part in halves:
        half = part.shape[1] // 2
        got = swap_tp(part[:, half:].astype(BF16), 1)
        part = part[:, :half] + got.astype(F32)
        half = half // 2
        got = swap_tp(part[:, half:].astype(BF16), 2)
        out.append(part[:, :half] + got.astype(F32))
    return jnp.concatenate(out, axis=-1)


def row_offsets(idx, rows, y, c):
    ec = idx // (2 * rows)
    ey = (idx // rows) % 2
    return ((ey ^ y) * 2 + (ec ^ c)) * rows + idx % rows


def fill_bias(bias_ref, tab_ref, s, n_blocks, block, rows):
    y = tab_ref[s, n_blocks + 2]
    c = tab_ref[s, n_blocks + 3]
    prefix = tab_ref[s, n_blocks + 1]
    koff = row_offsets(lax.broadcasted_iota(jnp.int32, (block, block), 0), rows, y, c)
    qoff = row_offsets(lax.broadcasted_iota(jnp.int32, (block, block), 1), rows, y, c)
    qpos = qoff + tab_ref[s, n_blocks] * block
    for kb in range(n_blocks):
        kpos = koff + tab_ref[s, kb] * block
        ok = (kpos <= qpos) | (kpos < prefix)
        bias_ref[kb * block : (kb + 1) * block, :] = jnp.where(ok, 0.0, NEG)


def fwd_kernel(n_blocks, block, rows, step, tab_ref, q_ref, kv_ref, vt_ref, o_ref, lse_ref, bias_ref):
    s = pl.program_id(0)

    @pl.when(pl.program_id(1) == 0)
    def _():
        fill_bias(bias_ref, tab_ref, s, n_blocks, block, rows)

    q = q_ref[...]
    qz = jnp.concatenate([q, jnp.zeros_like(q)], axis=0)
    seq = n_blocks * block
    m = jnp.full((1, block), -jnp.inf, F32)
    l = jnp.zeros((1, block), F32)
    acc = jnp.zeros((HD, block), F32)
    for k0 in range(0, seq, step):
        sc = dot(kv_ref[k0 : k0 + step, :], qz, 1, 0) + bias_ref[k0 : k0 + step, :]
        m_new = jnp.maximum(m, jnp.max(sc, axis=0, keepdims=True))
        alpha = jnp.exp(m - m_new)
        p = jnp.exp(sc - m_new)
        l = l * alpha + jnp.sum(p, axis=0, keepdims=True)
        acc = acc * alpha + dot(vt_ref[:, k0 : k0 + step], p.astype(BF16), 1, 0)
        m = m_new
    o_ref[...] = (acc / l).astype(BF16)
    lse_ref[0] = m + jnp.log(l)


def bwd_kernel(
    n_blocks, block, rows, step, tab_ref, q_ref, kv_ref, kt_ref, go_ref, o_ref, lse_ref,
    dq_ref, dkv_ref, bias_ref, dkv_acc,
):
    s = pl.program_id(0)
    h = pl.program_id(1)

    @pl.when(h == 0)
    def _():
        fill_bias(bias_ref, tab_ref, s, n_blocks, block, rows)
        dkv_acc[...] = jnp.zeros_like(dkv_acc)

    q = q_ref[...]
    go = go_ref[...]
    zero = jnp.zeros_like(q)
    qz = jnp.concatenate([q, zero], axis=0)
    gz = jnp.concatenate([zero, go], axis=0)
    lse = lse_ref[0]
    delta = jnp.sum(go.astype(F32) * o_ref[...].astype(F32), axis=0, keepdims=True)
    seq = n_blocks * block
    dq = jnp.zeros((HD, block), F32)
    for k0 in range(0, seq, step):
        ks = slice(k0, k0 + step)
        kv = kv_ref[ks, :]
        p = jnp.exp(dot(kv, qz, 1, 0) + bias_ref[ks, :] - lse)
        ds = (p * (dot(kv, gz, 1, 0) - delta)).astype(BF16)
        dkv_acc[HD:, ks] += dot(go, p.astype(BF16), 1, 1)
        dkv_acc[:HD, ks] += dot(q, ds, 1, 1)
        dq = dq + dot(kt_ref[:, ks], ds, 1, 0)
    dq_ref[...] = dq

    @pl.when(h == pl.num_programs(1) - 1)
    def _():
        dkv_ref[...] = dkv_acc[...].T.astype(BF16)


def attention_specs(n_blocks, block):
    seq = n_blocks * block
    q_spec = pl.BlockSpec((HD, block), lambda s, h, t: (h, s))
    kv_spec = pl.BlockSpec((seq, 2 * HD), lambda s, h, t: (0, s))
    lse_spec = pl.BlockSpec((1, 1, block), lambda s, h, t: (h, 0, s))

    def half_spec(which):
        return pl.BlockSpec((HD, seq), lambda s, h, t: (2 * s + which, 0))

    return q_spec, kv_spec, lse_spec, half_spec


def attention_forward(tab, q_t, kv, kv_t, n_blocks, block, rows):
    heads, seqs, seq = q_t.shape[0] // HD, q_t.shape[1] // block, n_blocks * block
    q_spec, kv_spec, lse_spec, half_spec = attention_specs(n_blocks, block)
    return pl.pallas_call(
        functools.partial(fwd_kernel, n_blocks, block, rows, min(512, seq)),
        name="attn_fwd",
        out_shape=(
            jax.ShapeDtypeStruct(q_t.shape, BF16),
            jax.ShapeDtypeStruct((heads, 1, seqs * block), F32),
        ),
        grid_spec=pltpu.PrefetchScalarGridSpec(
            num_scalar_prefetch=1,
            grid=(seqs, heads),
            in_specs=[q_spec, kv_spec, half_spec(1)],
            out_specs=[q_spec, lse_spec],
            scratch_shapes=[pltpu.VMEM((seq, block), F32)],
        ),
        compiler_params=pltpu.CompilerParams(
            dimension_semantics=("arbitrary", "arbitrary"), vmem_limit_bytes=48 << 20
        ),
        cost_estimate=pl.CostEstimate(
            flops=16 * heads * seqs * block * seq * HD,
            bytes_accessed=4 * seqs * seq * 2 * HD,
            transcendentals=heads * seqs * block * seq,
        ),
    )(tab, q_t, kv, kv_t)


def attention_backward(tab, q_t, kv, kv_t, go_t, o_t, lse, n_blocks, block, rows):
    heads, seqs, seq = q_t.shape[0] // HD, q_t.shape[1] // block, n_blocks * block
    q_spec, kv_spec, lse_spec, half_spec = attention_specs(n_blocks, block)
    return pl.pallas_call(
        functools.partial(bwd_kernel, n_blocks, block, rows, min(512, seq)),
        name="attn_bwd",
        out_shape=(
            jax.ShapeDtypeStruct(q_t.shape, F32),
            jax.ShapeDtypeStruct((seq, seqs * 2 * HD), BF16),
        ),
        grid_spec=pltpu.PrefetchScalarGridSpec(
            num_scalar_prefetch=1,
            grid=(seqs, heads),
            in_specs=[q_spec, kv_spec, half_spec(0), q_spec, q_spec, lse_spec],
            out_specs=[q_spec, kv_spec],
            scratch_shapes=[pltpu.VMEM((seq, block), F32), pltpu.VMEM((2 * HD, seq), F32)],
        ),
        compiler_params=pltpu.CompilerParams(
            dimension_semantics=("arbitrary", "arbitrary"), vmem_limit_bytes=48 << 20
        ),
        cost_estimate=pl.CostEstimate(
            flops=40 * heads * seqs * block * seq * HD,
            bytes_accessed=8 * seqs * seq * 2 * HD,
            transcendentals=heads * seqs * block * seq,
        ),
    )(tab, q_t, kv, kv_t, go_t, o_t, lse)


def on_device(
    hidden_in, cotangent, gain_attn, w_query, w_key, w_value, w_out, gain_mlp, w_gate, w_up,
    w_down, prefix, block_order,
):
    seqs, rows, width = hidden_in.shape
    n_tp = lax.axis_size("tp")
    n_fsdp = lax.axis_size("fsdp")
    if n_tp != 4 or n_fsdp % 2 or w_key.shape[1] != HD:
        raise ValueError("unsupported mesh")
    n_a = n_fsdp // 2
    block = rows * n_tp
    tokens = seqs * block
    half = width // 2
    chunk = width // n_fsdp
    q_width = w_query.shape[1]
    ff = w_gate.shape[1]
    fsdp_index = lax.axis_index("fsdp")
    a_idx, b_idx = fsdp_index // 2, fsdp_index % 2
    tp_index = lax.axis_index("tp")
    y_idx, c_idx = tp_index // 2, tp_index % 2
    first = b_idx == 0

    def to_rel(v):
        v = v.reshape(v.shape[:-1] + (n_a, 2, chunk))
        even, odd = v[..., 0, :], v[..., 1, :]
        lo = jnp.where(first, even, odd).reshape(v.shape[:-3] + (half,))
        hi = jnp.where(first, odd, even).reshape(v.shape[:-3] + (half,))
        return jnp.concatenate([lo, hi], axis=-1)

    def from_rel(v):
        lo = v[..., :half].reshape(v.shape[:-1] + (n_a, chunk))
        hi = v[..., half:].reshape(v.shape[:-1] + (n_a, chunk))
        even, odd = jnp.where(first, lo, hi), jnp.where(first, hi, lo)
        return jnp.stack([even, odd], axis=-2).reshape(v.shape[:-1] + (width,))

    gains = lax.all_gather(
        jnp.stack([gain_attn, gain_mlp]), ("fsdp", "tp"), axis=1, tiled=True
    )
    gains = to_rel(gains)
    gain_first, gain_second = gains[0], gains[1]
    own_block = jnp.sum(
        jnp.where(jnp.arange(n_fsdp)[None, :] == fsdp_index, block_order, 0), axis=1
    )
    by_b = block_order.reshape(seqs, n_a, 2)
    even, odd = by_b[:, :, 0], by_b[:, :, 1]
    key_blocks = jnp.concatenate(
        [jnp.where(first, even, odd), jnp.where(first, odd, even)], axis=1
    )
    tab = jnp.concatenate(
        [
            key_blocks,
            own_block[:, None],
            prefix[:, None],
            jnp.broadcast_to(y_idx, (seqs, 1)),
            jnp.broadcast_to(c_idx, (seqs, 1)),
        ],
        axis=1,
    ).astype(jnp.int32)
    lane = jnp.arange(block, dtype=jnp.int32)
    offs = row_offsets(lane, rows, y_idx, c_idx)
    pos = (own_block[:, None] * block + offs[None, :]).reshape(tokens)
    frequency = THETA ** (-(jnp.arange(HD // 2, dtype=F32) * 2.0 / HD))
    angles = frequency[:, None] * pos.astype(F32)[None, :]
    cos_t = jnp.cos(angles)[None]
    sin_t = jnp.sin(angles)[None]

    def rotate_t(v):
        v = v.reshape(-1, HD, tokens)
        u1, u2 = v[:, : HD // 2], v[:, HD // 2 :]
        return jnp.concatenate(
            [u1 * cos_t - u2 * sin_t, u2 * cos_t + u1 * sin_t], axis=1
        ).reshape(-1, tokens)

    def rotate_back_t(v):
        v = v.reshape(-1, HD, tokens)
        u1, u2 = v[:, : HD // 2], v[:, HD // 2 :]
        return jnp.concatenate(
            [u1 * cos_t + u2 * sin_t, u2 * cos_t - u1 * sin_t], axis=1
        ).reshape(-1, tokens)

    qkv_a, qkv_b = gather_halves(jnp.concatenate([w_query, w_key, w_value], axis=1))
    out_a, out_b = gather_halves(w_out.T)
    gu_a, gu_b = gather_halves(jnp.concatenate([w_gate, w_up], axis=1))
    down_a, down_b = gather_halves(w_down.T)

    x_rel = to_rel(hidden_in)
    x_all = spread_rows(x_rel).astype(F32)
    h_first = (x_all * inverse_rms(x_all) * gain_first).astype(BF16).reshape(tokens, width)
    gm = spread_rows(to_rel(cotangent).astype(BF16)).reshape(tokens, width)
    qkv_t = dot(qkv_a, h_first[:, :half], 0, 1) + dot(qkv_b, h_first[:, half:], 0, 1)
    q_t = (rotate_t(qkv_t[:q_width]).astype(BF16) * (HD**-0.5)).astype(BF16)
    kv_t = jnp.concatenate(
        [rotate_t(qkv_t[q_width : q_width + HD]), qkv_t[q_width + HD :]], axis=0
    ).astype(BF16)
    kv_own = (
        kv_t.reshape(2 * HD, seqs, block).transpose(2, 1, 0).reshape(block, seqs * 2 * HD)
    )
    kv = jnp.concatenate(gather_halves(kv_own), axis=0)
    kv_all_t = kv.T
    o_t, lse = attention_forward(tab, q_t, kv, kv_all_t, n_fsdp, block, rows)

    x_own = x_rel.astype(F32)
    rms_first = inverse_rms(x_own)

    def rows3(v):
        return v.reshape(seqs, block, half)

    middle = x_own + collect_rows(
        [rows3(dot(o_t, out_a, 0, 1)), rows3(dot(o_t, out_b, 0, 1))]
    )
    rms_second = inverse_rms(middle)
    h_second = spread_rows((middle * rms_second * gain_second).astype(BF16)).reshape(
        tokens, width
    )

    gu = dot(h_second[:, :half], gu_a, 1, 0) + dot(h_second[:, half:], gu_b, 1, 0)
    gate, up = gu[:, :ff], gu[:, ff:]
    sig = jax.nn.sigmoid(gate)
    hidden = (gate * sig * up).astype(BF16)
    g_hidden = dot(gm[:, :half], down_a, 1, 0) + dot(gm[:, half:], down_b, 1, 0)
    g_cat = jnp.concatenate(
        [
            (g_hidden * up * sig * (1.0 + gate * (1.0 - sig))).astype(BF16),
            (g_hidden * gate * sig).astype(BF16),
        ],
        axis=1,
    )
    g_h2 = collect_rows([rows3(dot(g_cat, gu_a, 1, 1)), rows3(dot(g_cat, gu_b, 1, 1))])
    down_g = scatter_halves(
        dot(gm[:, half:], hidden, 0, 0), lambda: dot(gm[:, :half], hidden, 0, 0)
    )
    gu_g = scatter_halves(
        dot(h_second[:, half:], g_cat, 0, 0), lambda: dot(h_second[:, :half], g_cat, 0, 0)
    )
    layer_out = middle + collect_rows(
        [rows3(dot(hidden, down_a, 1, 1)), rows3(dot(hidden, down_b, 1, 1))]
    )
    g_mid_norm, gain_second_sum = norm_back(g_h2, middle, gain_second, rms_second)
    g_mid = to_rel(cotangent) + g_mid_norm

    ga = spread_rows(g_mid.astype(BF16)).reshape(tokens, width)
    go_t = (dot(out_a, ga[:, :half], 0, 1) + dot(out_b, ga[:, half:], 0, 1)).astype(BF16)
    dq_t, dkv = attention_backward(
        tab, q_t, kv, kv_all_t, go_t, o_t, lse, n_fsdp, block, rows
    )
    out_g = scatter_halves(dot(ga[:, half:], o_t, 0, 1), lambda: dot(ga[:, :half], o_t, 0, 1))
    seq_half = n_a * block
    dkv_own = scatter_halves(
        dkv[seq_half:], lambda: dkv[:seq_half].astype(F32)
    ).astype(F32)
    dkv_t = dkv_own.reshape(block, seqs, 2 * HD).transpose(2, 1, 0).reshape(2 * HD, tokens)
    gq_t = rotate_back_t(dq_t * (HD**-0.5)).astype(BF16)
    gk_t = rotate_back_t(dkv_t[:HD]).astype(BF16)
    g_qkv_t = jnp.concatenate([gq_t, gk_t, dkv_t[HD:].astype(BF16)], axis=0)
    qkv_g = scatter_halves(
        dot(h_first[:, half:], g_qkv_t, 0, 1), lambda: dot(h_first[:, :half], g_qkv_t, 0, 1)
    )
    g_h1 = collect_rows([rows3(dot(g_qkv_t, qkv_a, 0, 1)), rows3(dot(g_qkv_t, qkv_b, 0, 1))])
    g_in_norm, gain_first_sum = norm_back(g_h1, x_own, gain_first, rms_first)
    g_in = g_mid + g_in_norm
    gain_sums = lax.psum_scatter(
        from_rel(jnp.stack([gain_first_sum, gain_second_sum])),
        ("fsdp", "tp"),
        scatter_dimension=1,
        tiled=True,
    )
    qkv_g = qkv_g.astype(F32)
    gu_g = gu_g.astype(F32)
    return (
        from_rel(layer_out),
        from_rel(g_in),
        gain_sums[0],
        qkv_g[:, :q_width],
        qkv_g[:, q_width : q_width + HD],
        qkv_g[:, q_width + HD :],
        out_g.astype(F32).T,
        gain_sums[1],
        gu_g[:, :ff],
        gu_g[:, ff:],
        down_g.astype(F32).T,
    )


def solution(mesh):
    rows = P(None, ("fsdp", "tp"), None)
    gain = P(("fsdp", "tp"))
    col = P("fsdp", "tp")
    row = P("tp", "fsdp")
    return jax.shard_map(
        on_device,
        mesh=mesh,
        in_specs=(rows, rows, gain, col, col, col, row, gain, col, col, row, P(), P()),
        out_specs=(rows, rows, gain, col, col, col, row, gain, col, col, row),
        check_vma=False,
    )
```

```python
import functools

import jax
import jax.numpy as jnp
from jax import lax
from jax.experimental import pallas as pl
from jax.experimental.pallas import tpu as pltpu
from jax.sharding import PartitionSpec as P

HD = 64
EPS = 1e-05
THETA = 10000.0
NEG = -1000000000.0
F32 = jnp.float32
BF16 = jnp.bfloat16


def inverse_rms(values):
    return lax.rsqrt(jnp.mean(values * values, axis=-1, keepdims=True) + EPS)


def norm_back(upstream, values, gain_vec, inv_rms):
    weighted = upstream * gain_vec
    inner_mean = jnp.mean(weighted * values, axis=-1, keepdims=True)
    return (
        inv_rms * weighted - values * (inv_rms * inv_rms * inv_rms) * inner_mean,
        jnp.sum(upstream * values * inv_rms, axis=(0, 1)),
    )


def dot(a, b, ca, cb):
    return lax.dot_general(a, b, (((ca,), (cb,)), ((), ())), preferred_element_type=F32)


def swap_b(v):
    n = lax.axis_size("fsdp")
    return lax.ppermute(v, "fsdp", [(i, i ^ 1) for i in range(n)])


def a_groups():
    n = lax.axis_size("fsdp")
    return [[b + 2 * a for a in range(n // 2)] for b in range(2)]


def gather_halves(shard):
    own = lax.all_gather(shard, "fsdp", axis=0, tiled=True, axis_index_groups=a_groups())
    return own, swap_b(own)


def scatter_halves(send, keep_fn):
    other = swap_b(send.astype(BF16))
    total = (keep_fn() + other.astype(F32)).astype(BF16)
    return lax.psum_scatter(
        total, "fsdp", scatter_dimension=0, tiled=True, axis_index_groups=a_groups()
    )


def swap_tp(v, bit):
    n = lax.axis_size("tp")
    return lax.ppermute(v, "tp", [(i, i ^ bit) for i in range(n)])


def spread_rows(v):
    pair = jnp.concatenate([v, swap_tp(v, 2)], axis=1)
    return jnp.concatenate([pair, swap_tp(pair, 1)], axis=1)


def collect_rows(halves):
    out = []
    for part in halves:
        half = part.shape[1] // 2
        got = swap_tp(part[:, half:].astype(BF16), 1)
        part = part[:, :half] + got.astype(F32)
        half = half // 2
        got = swap_tp(part[:, half:].astype(BF16), 2)
        out.append(part[:, :half] + got.astype(F32))
    return jnp.concatenate(out, axis=-1)


MESH_ID = pl.DeviceIdType.MESH
HBM_SPEC = pl.BlockSpec(memory_space=pl.ANY)
VMEM_SPEC = pl.BlockSpec(memory_space=pltpu.VMEM)


def remote(src, dst, send, recv, fsdp, tp):
    return pltpu.make_async_remote_copy(
        src_ref=src,
        dst_ref=dst,
        send_sem=send,
        recv_sem=recv,
        device_id=(fsdp, tp),
        device_id_type=MESH_ID,
    )


def greet(peers):
    barrier = pltpu.get_barrier_semaphore()
    for fsdp, tp in peers:
        pl.semaphore_signal(barrier, inc=1, device_id=(fsdp, tp), device_id_type=MESH_ID)
    pl.semaphore_wait(barrier, len(peers))


def coords(n_a):
    fsdp, tp = lax.axis_index("fsdp"), lax.axis_index("tp")
    return fsdp // 2, fsdp % 2, tp


class FsdpGather:
    def __init__(self, n_a, own, out, sems):
        self.n_a, self.own, self.out = n_a, own, out
        self.z_send, self.z_recv, self.x_send, self.x_recv, self.local = sems

    def z_copy(self, d):
        a, b, tp = coords(self.n_a)
        to = lax.rem(a + d, self.n_a)
        return remote(
            self.own, self.out.at[0, a], self.z_send.at[d], self.z_recv.at[d], to * 2 + b, tp
        )

    def x_copy(self, d):
        a, b, tp = coords(self.n_a)
        at = lax.rem(a + self.n_a - d, self.n_a)
        src = self.own if d == 0 else self.out.at[0, at]
        return remote(
            src, self.out.at[1, at], self.x_send.at[d], self.x_recv.at[d], a * 2 + 1 - b, tp
        )

    def start(self):
        a, _, _ = coords(self.n_a)
        self.x_copy(0).start()
        for d in range(1, self.n_a):
            self.z_copy(d).start()
        pltpu.make_async_copy(self.own, self.out.at[0, a], self.local).start()

    def forward(self):
        for d in range(1, self.n_a):
            self.z_copy(d).wait_recv()
            self.x_copy(d).start()

    def finish(self):
        a, _, _ = coords(self.n_a)
        for d in range(1, self.n_a):
            self.z_copy(d).wait_send()
        for d in range(self.n_a):
            self.x_copy(d).wait()
        pltpu.make_async_copy(self.own, self.out.at[0, a], self.local).wait()


def gather_sems(n_a):
    dma = pltpu.SemaphoreType.DMA
    return [dma((n_a,)), dma((n_a,)), dma((n_a,)), dma((n_a,)), dma(())]


def fsdp_peers(n_a):
    a, b, tp = coords(n_a)
    peers = [(a * 2 + 1 - b, tp)]
    return peers + [(lax.rem(a + d, n_a) * 2 + b, tp) for d in range(1, n_a)]


def prologue_kernel(
    n_a, w_ref, x_ref, g_ref, wall_ref, xall_ref, gall_ref,
    s0, s1, s2, s3, s4, tp_send, tp_recv, tp_local, g_send, g_recv,
):
    a, b, tp = coords(n_a)
    fsdp = a * 2 + b
    n_dev = n_a * 8
    me = fsdp * 4 + tp
    barrier = pltpu.get_barrier_semaphore()

    def peer(k):
        p = lax.rem(me + k, n_dev)
        return p // 4, p % 4

    @pl.loop(1, n_dev)
    def _(k):
        pl.semaphore_signal(barrier, inc=1, device_id=peer(k), device_id_type=MESH_ID)

    pl.semaphore_wait(barrier, n_dev - 1)

    def gain_copy(k):
        f, t = peer(k)
        return remote(g_ref, gall_ref.at[me], g_send.at[k], g_recv.at[k], f, t)

    gather = FsdpGather(n_a, w_ref, wall_ref, (s0, s1, s2, s3, s4))
    y_tp = lax.rem(tp + 2, 4)
    c_tp = tp + 1 - 2 * (tp % 2)
    to_y = remote(x_ref, xall_ref.at[:, 1], tp_send.at[0], tp_recv.at[0], fsdp, y_tp)
    to_c = remote(x_ref, xall_ref.at[:, 2], tp_send.at[1], tp_recv.at[1], fsdp, c_tp)
    fwd = remote(
        xall_ref.at[:, 1], xall_ref.at[:, 3], tp_send.at[2], tp_recv.at[2], fsdp, c_tp
    )
    mine = pltpu.make_async_copy(x_ref, xall_ref.at[:, 0], tp_local)

    @pl.loop(1, n_dev)
    def _(k):
        gain_copy(k).start()

    gather.start()
    to_y.start()
    to_c.start()
    mine.start()
    gall_ref[me] = g_ref[...]
    to_y.wait_recv()
    fwd.start()
    gather.forward()

    @pl.loop(1, n_dev)
    def _(k):
        gain_copy(k).wait()

    to_y.wait_send()
    to_c.wait()
    fwd.wait()
    mine.wait()
    gather.finish()


def prologue(w, x, gains):
    n_a = lax.axis_size("fsdp") // 2
    n_dev = n_a * 8
    dma = pltpu.SemaphoreType.DMA
    seqs, rows, width = x.shape
    return pl.pallas_call(
        functools.partial(prologue_kernel, n_a),
        name="prologue",
        out_shape=(
            jax.ShapeDtypeStruct((2, n_a) + w.shape, w.dtype),
            jax.ShapeDtypeStruct((seqs, 4, rows, width), x.dtype),
            jax.ShapeDtypeStruct((n_dev,) + gains.shape, gains.dtype),
        ),
        in_specs=[VMEM_SPEC] * 3,
        out_specs=(HBM_SPEC, HBM_SPEC, VMEM_SPEC),
        scratch_shapes=gather_sems(n_a)
        + [dma((3,)), dma((3,)), dma(()), dma((n_dev,)), dma((n_dev,))],
        compiler_params=pltpu.CompilerParams(collective_id=1, has_side_effects=True),
        cost_estimate=pl.CostEstimate(flops=0, bytes_accessed=40 << 20, transcendentals=0),
    )(w, x, gains)


def gather_kernel(n_a, own_ref, out_ref, *sems):
    greet(fsdp_peers(n_a))
    gather = FsdpGather(n_a, own_ref, out_ref, sems)
    gather.start()
    gather.forward()
    gather.finish()


def gather_blocks(own):
    n_a = lax.axis_size("fsdp") // 2
    return pl.pallas_call(
        functools.partial(gather_kernel, n_a),
        name="kv_gather",
        out_shape=jax.ShapeDtypeStruct((2, n_a) + own.shape, own.dtype),
        in_specs=[VMEM_SPEC],
        out_specs=HBM_SPEC,
        scratch_shapes=gather_sems(n_a),
        compiler_params=pltpu.CompilerParams(collective_id=2, has_side_effects=True),
        cost_estimate=pl.CostEstimate(flops=0, bytes_accessed=40 << 20, transcendentals=0),
    )(own)


def scatter_kernel(n_a, part_ref, out_ref, got, send, recv):
    a, b, tp = coords(n_a)
    peers = [
        (e, d, lax.rem(a + d, n_a), lax.rem(b + e, 2))
        for d in range(n_a)
        for e in range(2)
        if (d, e) != (0, 0)
    ]
    greet([(pa * 2 + pb, tp) for _, _, pa, pb in peers])
    copies = [
        remote(
            part_ref.at[e, pa], got.at[2 * d + e - 1], send.at[2 * d + e - 1],
            recv.at[2 * d + e - 1], pa * 2 + pb, tp,
        )
        for e, d, pa, pb in peers
    ]
    for copy in copies:
        copy.start()
    total = part_ref[0, a].astype(F32)
    for i, copy in enumerate(copies):
        copy.wait_recv()
        total = total + got[i].astype(F32)
    out_ref[...] = total
    for copy in copies:
        copy.wait_send()


def scatter_blocks(part):
    n_a = part.shape[1]
    n = 2 * n_a - 1
    dma = pltpu.SemaphoreType.DMA
    return pl.pallas_call(
        functools.partial(scatter_kernel, n_a),
        name="kv_scatter",
        out_shape=jax.ShapeDtypeStruct(part.shape[2:], F32),
        in_specs=[VMEM_SPEC],
        out_specs=VMEM_SPEC,
        scratch_shapes=[pltpu.VMEM((n,) + part.shape[2:], part.dtype), dma((n,)), dma((n,))],
        compiler_params=pltpu.CompilerParams(
            collective_id=3, has_side_effects=True, vmem_limit_bytes=48 << 20
        ),
        cost_estimate=pl.CostEstimate(flops=0, bytes_accessed=40 << 20, transcendentals=0),
    )(part)


def gain_kernel(n_a, part_ref, out_ref, got, send, recv):
    a, b, tp = coords(n_a)
    n_dev = n_a * 8
    me = (a * 2 + b) * 4 + tp
    barrier = pltpu.get_barrier_semaphore()

    def peer(k):
        return lax.rem(me + k, n_dev)

    @pl.loop(1, n_dev)
    def _(k):
        p = peer(k)
        pl.semaphore_signal(barrier, inc=1, device_id=(p // 4, p % 4), device_id_type=MESH_ID)

    pl.semaphore_wait(barrier, n_dev - 1)

    def copy(k):
        p = peer(k)
        return remote(part_ref.at[p], got.at[k], send.at[k], recv.at[k], p // 4, p % 4)

    @pl.loop(1, n_dev)
    def _(k):
        copy(k).start()

    got[0] = part_ref[me]

    @pl.loop(1, n_dev)
    def _(k):
        copy(k).wait()

    out_ref[...] = jnp.sum(got[...], axis=0)


def scatter_gains(part):
    n_a = lax.axis_size("fsdp") // 2
    dma = pltpu.SemaphoreType.DMA
    n = part.shape[0]
    return pl.pallas_call(
        functools.partial(gain_kernel, n_a),
        name="gain_scatter",
        out_shape=jax.ShapeDtypeStruct(part.shape[1:], F32),
        in_specs=[VMEM_SPEC],
        out_specs=VMEM_SPEC,
        scratch_shapes=[pltpu.VMEM(part.shape, F32), dma((n,)), dma((n,))],
        compiler_params=pltpu.CompilerParams(collective_id=4, has_side_effects=True),
    )(part)


def row_offsets(idx, rows, y, c):
    ec = idx // (2 * rows)
    ey = (idx // rows) % 2
    return ((ey ^ y) * 2 + (ec ^ c)) * rows + idx % rows


def fill_bias(bias_ref, tab_ref, s, n_blocks, block, rows):
    y = tab_ref[s, n_blocks + 2]
    c = tab_ref[s, n_blocks + 3]
    prefix = tab_ref[s, n_blocks + 1]
    koff = row_offsets(lax.broadcasted_iota(jnp.int32, (block, block), 0), rows, y, c)
    qoff = row_offsets(lax.broadcasted_iota(jnp.int32, (block, block), 1), rows, y, c)
    qpos = qoff + tab_ref[s, n_blocks] * block
    for kb in range(n_blocks):
        kpos = koff + tab_ref[s, kb] * block
        ok = (kpos <= qpos) | (kpos < prefix)
        bias_ref[kb * block : (kb + 1) * block, :] = jnp.where(ok, 0.0, NEG)


def fwd_kernel(n_blocks, block, rows, step, tab_ref, q_ref, kv_ref, vt_ref, o_ref, lse_ref, bias_ref):
    s = pl.program_id(0)

    @pl.when(pl.program_id(1) == 0)
    def _():
        fill_bias(bias_ref, tab_ref, s, n_blocks, block, rows)

    q = q_ref[...]
    qz = jnp.concatenate([q, jnp.zeros_like(q)], axis=0)
    seq = n_blocks * block
    m = jnp.full((1, block), -jnp.inf, F32)
    l = jnp.zeros((1, block), F32)
    acc = jnp.zeros((HD, block), F32)
    for k0 in range(0, seq, step):
        sc = dot(kv_ref[k0 : k0 + step, :], qz, 1, 0) + bias_ref[k0 : k0 + step, :]
        m_new = jnp.maximum(m, jnp.max(sc, axis=0, keepdims=True))
        alpha = jnp.exp(m - m_new)
        p = jnp.exp(sc - m_new)
        l = l * alpha + jnp.sum(p, axis=0, keepdims=True)
        acc = acc * alpha + dot(vt_ref[:, k0 : k0 + step], p.astype(BF16), 1, 0)
        m = m_new
    o_ref[...] = (acc / l).astype(BF16)
    lse_ref[0] = m + jnp.log(l)


def bwd_kernel(
    n_blocks, block, rows, step, tab_ref, q_ref, kv_ref, kt_ref, go_ref, o_ref, lse_ref,
    dq_ref, dkv_ref, bias_ref, dkv_acc,
):
    s = pl.program_id(0)
    h = pl.program_id(1)

    @pl.when(h == 0)
    def _():
        fill_bias(bias_ref, tab_ref, s, n_blocks, block, rows)
        dkv_acc[...] = jnp.zeros_like(dkv_acc)

    q = q_ref[...]
    go = go_ref[...]
    zero = jnp.zeros_like(q)
    qz = jnp.concatenate([q, zero], axis=0)
    gz = jnp.concatenate([zero, go], axis=0)
    lse = lse_ref[0]
    delta = jnp.sum(go.astype(F32) * o_ref[...].astype(F32), axis=0, keepdims=True)
    seq = n_blocks * block
    dq = jnp.zeros((HD, block), F32)
    for k0 in range(0, seq, step):
        ks = slice(k0, k0 + step)
        kv = kv_ref[ks, :]
        p = jnp.exp(dot(kv, qz, 1, 0) + bias_ref[ks, :] - lse)
        ds = (p * (dot(kv, gz, 1, 0) - delta)).astype(BF16)
        dkv_acc[HD:, ks] += dot(go, p.astype(BF16), 1, 1)
        dkv_acc[:HD, ks] += dot(q, ds, 1, 1)
        dq = dq + dot(kt_ref[:, ks], ds, 1, 0)
    dq_ref[...] = dq

    @pl.when(h == pl.num_programs(1) - 1)
    def _():
        dkv_ref[...] = dkv_acc[...].T.astype(BF16)


def attention_specs(n_blocks, block):
    seq = n_blocks * block
    q_spec = pl.BlockSpec((HD, block), lambda s, h, t: (h, s))
    kv_spec = pl.BlockSpec((seq, 2 * HD), lambda s, h, t: (0, s))
    lse_spec = pl.BlockSpec((1, 1, block), lambda s, h, t: (h, 0, s))

    def half_spec(which):
        return pl.BlockSpec((HD, seq), lambda s, h, t: (2 * s + which, 0))

    return q_spec, kv_spec, lse_spec, half_spec


def attention_forward(tab, q_t, kv, kv_t, n_blocks, block, rows):
    heads, seqs, seq = q_t.shape[0] // HD, q_t.shape[1] // block, n_blocks * block
    q_spec, kv_spec, lse_spec, half_spec = attention_specs(n_blocks, block)
    return pl.pallas_call(
        functools.partial(fwd_kernel, n_blocks, block, rows, min(512, seq)),
        name="attn_fwd",
        out_shape=(
            jax.ShapeDtypeStruct(q_t.shape, BF16),
            jax.ShapeDtypeStruct((heads, 1, seqs * block), F32),
        ),
        grid_spec=pltpu.PrefetchScalarGridSpec(
            num_scalar_prefetch=1,
            grid=(seqs, heads),
            in_specs=[q_spec, kv_spec, half_spec(1)],
            out_specs=[q_spec, lse_spec],
            scratch_shapes=[pltpu.VMEM((seq, block), F32)],
        ),
        compiler_params=pltpu.CompilerParams(
            dimension_semantics=("arbitrary", "arbitrary"), vmem_limit_bytes=48 << 20
        ),
        cost_estimate=pl.CostEstimate(
            flops=16 * heads * seqs * block * seq * HD,
            bytes_accessed=4 * seqs * seq * 2 * HD,
            transcendentals=heads * seqs * block * seq,
        ),
    )(tab, q_t, kv, kv_t)


def attention_backward(tab, q_t, kv, kv_t, go_t, o_t, lse, n_blocks, block, rows):
    heads, seqs, seq = q_t.shape[0] // HD, q_t.shape[1] // block, n_blocks * block
    q_spec, kv_spec, lse_spec, half_spec = attention_specs(n_blocks, block)
    return pl.pallas_call(
        functools.partial(bwd_kernel, n_blocks, block, rows, min(512, seq)),
        name="attn_bwd",
        out_shape=(
            jax.ShapeDtypeStruct(q_t.shape, F32),
            jax.ShapeDtypeStruct((seq, seqs * 2 * HD), BF16),
        ),
        grid_spec=pltpu.PrefetchScalarGridSpec(
            num_scalar_prefetch=1,
            grid=(seqs, heads),
            in_specs=[q_spec, kv_spec, half_spec(0), q_spec, q_spec, lse_spec],
            out_specs=[q_spec, kv_spec],
            scratch_shapes=[pltpu.VMEM((seq, block), F32), pltpu.VMEM((2 * HD, seq), F32)],
        ),
        compiler_params=pltpu.CompilerParams(
            dimension_semantics=("arbitrary", "arbitrary"), vmem_limit_bytes=48 << 20
        ),
        cost_estimate=pl.CostEstimate(
            flops=40 * heads * seqs * block * seq * HD,
            bytes_accessed=8 * seqs * seq * 2 * HD,
            transcendentals=heads * seqs * block * seq,
        ),
    )(tab, q_t, kv, kv_t, go_t, o_t, lse)


def on_device(
    hidden_in, cotangent, gain_attn, w_query, w_key, w_value, w_out, gain_mlp, w_gate, w_up,
    w_down, prefix, block_order,
):
    seqs, rows, width = hidden_in.shape
    n_tp = lax.axis_size("tp")
    n_fsdp = lax.axis_size("fsdp")
    if n_tp != 4 or n_fsdp % 2 or w_key.shape[1] != HD:
        raise ValueError("unsupported mesh")
    n_a = n_fsdp // 2
    block = rows * n_tp
    tokens = seqs * block
    half = width // 2
    chunk = width // n_fsdp
    q_width = w_query.shape[1]
    ff = w_gate.shape[1]
    fsdp_index = lax.axis_index("fsdp")
    a_idx, b_idx = fsdp_index // 2, fsdp_index % 2
    tp_index = lax.axis_index("tp")
    y_idx, c_idx = tp_index // 2, tp_index % 2
    first = b_idx == 0

    def to_rel(v):
        v = v.reshape(v.shape[:-1] + (n_a, 2, chunk))
        even, odd = v[..., 0, :], v[..., 1, :]
        lo = jnp.where(first, even, odd).reshape(v.shape[:-3] + (half,))
        hi = jnp.where(first, odd, even).reshape(v.shape[:-3] + (half,))
        return jnp.concatenate([lo, hi], axis=-1)

    def from_rel(v):
        lo = v[..., :half].reshape(v.shape[:-1] + (n_a, chunk))
        hi = v[..., half:].reshape(v.shape[:-1] + (n_a, chunk))
        even, odd = jnp.where(first, lo, hi), jnp.where(first, hi, lo)
        return jnp.stack([even, odd], axis=-2).reshape(v.shape[:-1] + (width,))

    x_rel = to_rel(hidden_in)
    piece = gain_attn.shape[0]
    fill = -2 * piece % 128
    gain_row = jnp.pad(jnp.concatenate([gain_attn, gain_mlp]), (0, fill))
    gain_row = jnp.broadcast_to(gain_row[None], (8, 2 * piece + fill))
    qkv_w, x_all, gains = prologue(
        jnp.concatenate([w_query, w_key, w_value], axis=1), x_rel, gain_row
    )
    gains = gains[:, 0]
    gain_first = to_rel(gains[:, :piece].reshape(width))
    gain_second = to_rel(gains[:, piece : 2 * piece].reshape(width))
    qkv_a = qkv_w[0].reshape(half, -1)
    qkv_b = qkv_w[1].reshape(half, -1)
    own_block = jnp.sum(
        jnp.where(jnp.arange(n_fsdp)[None, :] == fsdp_index, block_order, 0), axis=1
    )
    by_b = block_order.reshape(seqs, n_a, 2)
    even, odd = by_b[:, :, 0], by_b[:, :, 1]
    key_blocks = jnp.concatenate(
        [jnp.where(first, even, odd), jnp.where(first, odd, even)], axis=1
    )
    tab = jnp.concatenate(
        [
            key_blocks,
            own_block[:, None],
            prefix[:, None],
            jnp.broadcast_to(y_idx, (seqs, 1)),
            jnp.broadcast_to(c_idx, (seqs, 1)),
        ],
        axis=1,
    ).astype(jnp.int32)
    lane = jnp.arange(block, dtype=jnp.int32)
    offs = row_offsets(lane, rows, y_idx, c_idx)
    pos = (own_block[:, None] * block + offs[None, :]).reshape(tokens)
    frequency = THETA ** (-(jnp.arange(HD // 2, dtype=F32) * 2.0 / HD))
    angles = frequency[:, None] * pos.astype(F32)[None, :]
    cos_t = jnp.cos(angles)[None]
    sin_t = jnp.sin(angles)[None]

    def rotate_t(v):
        v = v.reshape(-1, HD, tokens)
        u1, u2 = v[:, : HD // 2], v[:, HD // 2 :]
        return jnp.concatenate(
            [u1 * cos_t - u2 * sin_t, u2 * cos_t + u1 * sin_t], axis=1
        ).reshape(-1, tokens)

    def rotate_back_t(v):
        v = v.reshape(-1, HD, tokens)
        u1, u2 = v[:, : HD // 2], v[:, HD // 2 :]
        return jnp.concatenate(
            [u1 * cos_t + u2 * sin_t, u2 * cos_t - u1 * sin_t], axis=1
        ).reshape(-1, tokens)

    out_a, out_b = gather_halves(w_out.T)
    gu_a, gu_b = gather_halves(jnp.concatenate([w_gate, w_up], axis=1))
    down_a, down_b = gather_halves(w_down.T)

    x_all = x_all.reshape(seqs, block, width).astype(F32)
    h_first = (x_all * inverse_rms(x_all) * gain_first).astype(BF16).reshape(tokens, width)
    gm = spread_rows(to_rel(cotangent).astype(BF16)).reshape(tokens, width)
    qkv_t = dot(qkv_a, h_first[:, :half], 0, 1) + dot(qkv_b, h_first[:, half:], 0, 1)
    q_t = (rotate_t(qkv_t[:q_width]).astype(BF16) * (HD**-0.5)).astype(BF16)
    kv_t = jnp.concatenate(
        [rotate_t(qkv_t[q_width : q_width + HD]), qkv_t[q_width + HD :]], axis=0
    ).astype(BF16)
    kv_own = (
        kv_t.reshape(2 * HD, seqs, block).transpose(2, 1, 0).reshape(block, seqs * 2 * HD)
    )
    kv = gather_blocks(kv_own).reshape(n_fsdp * block, -1)
    kv_all_t = kv.T
    o_t, lse = attention_forward(tab, q_t, kv, kv_all_t, n_fsdp, block, rows)

    x_own = x_rel.astype(F32)
    rms_first = inverse_rms(x_own)

    def rows3(v):
        return v.reshape(seqs, block, half)

    middle = x_own + collect_rows(
        [rows3(dot(o_t, out_a, 0, 1)), rows3(dot(o_t, out_b, 0, 1))]
    )
    rms_second = inverse_rms(middle)
    h_second = spread_rows((middle * rms_second * gain_second).astype(BF16)).reshape(
        tokens, width
    )

    gu = dot(h_second[:, :half], gu_a, 1, 0) + dot(h_second[:, half:], gu_b, 1, 0)
    gate, up = gu[:, :ff], gu[:, ff:]
    sig = jax.nn.sigmoid(gate)
    hidden = (gate * sig * up).astype(BF16)
    g_hidden = dot(gm[:, :half], down_a, 1, 0) + dot(gm[:, half:], down_b, 1, 0)
    g_cat = jnp.concatenate(
        [
            (g_hidden * up * sig * (1.0 + gate * (1.0 - sig))).astype(BF16),
            (g_hidden * gate * sig).astype(BF16),
        ],
        axis=1,
    )
    g_h2 = collect_rows([rows3(dot(g_cat, gu_a, 1, 1)), rows3(dot(g_cat, gu_b, 1, 1))])
    down_g = scatter_halves(
        dot(gm[:, half:], hidden, 0, 0), lambda: dot(gm[:, :half], hidden, 0, 0)
    )
    gu_g = scatter_halves(
        dot(h_second[:, half:], g_cat, 0, 0), lambda: dot(h_second[:, :half], g_cat, 0, 0)
    )
    layer_out = middle + collect_rows(
        [rows3(dot(hidden, down_a, 1, 1)), rows3(dot(hidden, down_b, 1, 1))]
    )
    g_mid_norm, gain_second_sum = norm_back(g_h2, middle, gain_second, rms_second)
    g_mid = to_rel(cotangent) + g_mid_norm

    ga = spread_rows(g_mid.astype(BF16)).reshape(tokens, width)
    go_t = (dot(out_a, ga[:, :half], 0, 1) + dot(out_b, ga[:, half:], 0, 1)).astype(BF16)
    dq_t, dkv = attention_backward(
        tab, q_t, kv, kv_all_t, go_t, o_t, lse, n_fsdp, block, rows
    )
    out_g = scatter_halves(dot(ga[:, half:], o_t, 0, 1), lambda: dot(ga[:, :half], o_t, 0, 1))
    dkv_own = scatter_blocks(dkv.reshape(2, n_a, block, -1))
    dkv_t = dkv_own.reshape(block, seqs, 2 * HD).transpose(2, 1, 0).reshape(2 * HD, tokens)
    gq_t = rotate_back_t(dq_t * (HD**-0.5)).astype(BF16)
    gk_t = rotate_back_t(dkv_t[:HD]).astype(BF16)
    g_qkv_t = jnp.concatenate([gq_t, gk_t, dkv_t[HD:].astype(BF16)], axis=0)
    qkv_g = scatter_halves(
        dot(h_first[:, half:], g_qkv_t, 0, 1), lambda: dot(h_first[:, :half], g_qkv_t, 0, 1)
    )
    g_h1 = collect_rows([rows3(dot(g_qkv_t, qkv_a, 0, 1)), rows3(dot(g_qkv_t, qkv_b, 0, 1))])
    g_in_norm, gain_first_sum = norm_back(g_h1, x_own, gain_first, rms_first)
    g_in = g_mid + g_in_norm
    gain_parts = jnp.concatenate(
        [
            from_rel(gain_first_sum).reshape(-1, piece),
            from_rel(gain_second_sum).reshape(-1, piece),
        ],
        axis=1,
    )
    gain_parts = jnp.pad(gain_parts, ((0, 0), (0, fill)))
    gain_parts = jnp.broadcast_to(
        gain_parts[:, None], (n_fsdp * 4, 8, 2 * piece + fill)
    )
    gain_sums = scatter_gains(gain_parts)[0]
    qkv_g = qkv_g.astype(F32)
    gu_g = gu_g.astype(F32)
    return (
        from_rel(layer_out),
        from_rel(g_in),
        gain_sums[:piece],
        qkv_g[:, :q_width],
        qkv_g[:, q_width : q_width + HD],
        qkv_g[:, q_width + HD :],
        out_g.astype(F32).T,
        gain_sums[piece : 2 * piece],
        gu_g[:, :ff],
        gu_g[:, ff:],
        down_g.astype(F32).T,
    )


def solution(mesh):
    rows = P(None, ("fsdp", "tp"), None)
    gain = P(("fsdp", "tp"))
    col = P("fsdp", "tp")
    row = P("tp", "fsdp")
    return jax.shard_map(
        on_device,
        mesh=mesh,
        in_specs=(rows, rows, gain, col, col, col, row, gain, col, col, row, P(), P()),
        out_specs=(rows, rows, gain, col, col, col, row, gain, col, col, row),
        check_vma=False,
    )
```

```python
import functools

import jax
import jax.numpy as jnp
from jax import lax
from jax.experimental import pallas as pl
from jax.experimental.pallas import tpu as pltpu
from jax.sharding import PartitionSpec as P

HD = 64
EPS = 1e-05
THETA = 10000.0
NEG = -1000000000.0
F32 = jnp.float32
BF16 = jnp.bfloat16


def inverse_rms(values):
    return lax.rsqrt(jnp.mean(values * values, axis=-1, keepdims=True) + EPS)


def norm_back(upstream, values, gain_vec, inv_rms):
    weighted = upstream * gain_vec
    inner_mean = jnp.mean(weighted * values, axis=-1, keepdims=True)
    return (
        inv_rms * weighted - values * (inv_rms * inv_rms * inv_rms) * inner_mean,
        jnp.sum(upstream * values * inv_rms, axis=0),
    )


def dot(a, b, ca, cb):
    return lax.dot_general(a, b, (((ca,), (cb,)), ((), ())), preferred_element_type=F32)


def swap_b(v):
    n = lax.axis_size("fsdp")
    return lax.ppermute(v, "fsdp", [(i, i ^ 1) for i in range(n)])


def swap_tp(v, bit):
    n = lax.axis_size("tp")
    return lax.ppermute(v, "tp", [(i, i ^ bit) for i in range(n)])


def a_groups():
    n = lax.axis_size("fsdp")
    return [[b + 2 * a for a in range(n // 2)] for b in range(2)]


def gather_a(shard):
    return lax.all_gather(shard, "fsdp", axis=0, tiled=True, axis_index_groups=a_groups())


def scatter_a(part):
    return lax.psum_scatter(
        part, "fsdp", scatter_dimension=0, tiled=True, axis_index_groups=a_groups()
    )


MESH_ID = pl.DeviceIdType.MESH
HBM_SPEC = pl.BlockSpec(memory_space=pl.ANY)
VMEM_SPEC = pl.BlockSpec(memory_space=pltpu.VMEM)
DMA = pltpu.SemaphoreType.DMA


def coords(n_a):
    fsdp, tp = lax.axis_index("fsdp"), lax.axis_index("tp")
    return fsdp // 2, fsdp % 2, tp


def remote(src, dst, sems, i, device):
    return pltpu.make_async_remote_copy(
        src_ref=src,
        dst_ref=dst,
        send_sem=sems[0].at[i],
        recv_sem=sems[1].at[i],
        device_id=device,
        device_id_type=MESH_ID,
    )


def greet(peers):
    barrier = pltpu.get_barrier_semaphore()
    for peer in peers:
        pl.semaphore_signal(barrier, inc=1, device_id=peer, device_id_type=MESH_ID)
    pl.semaphore_wait(barrier, len(peers))


def x_peer(n_a):
    a, b, tp = coords(n_a)
    return (a * 2 + 1 - b, tp)


def y_peer(n_a):
    a, b, tp = coords(n_a)
    return (a * 2 + b, lax.rem(tp + 2, 4))


def c_peer(n_a):
    a, b, tp = coords(n_a)
    return (a * 2 + b, tp + 1 - 2 * (tp % 2))


def a_peers(n_a):
    a, b, tp = coords(n_a)
    return [(lax.rem(a + d, n_a) * 2 + b, tp) for d in range(1, n_a)]


class FsdpGather:
    def __init__(self, n_a, own, out, slot, sems):
        self.n_a, self.own, self.out, self.slot = n_a, own, out, slot
        self.z, self.x, self.local = sems[:2], sems[2:4], sems[4]

    def at(self, e, a):
        i, j = self.slot(e, a)
        return self.out.at[i, j]

    def z_copy(self, d):
        a, _, _ = coords(self.n_a)
        return remote(self.own, self.at(0, a), self.z, d, a_peers(self.n_a)[d - 1])

    def x_copy(self, d):
        a, _, _ = coords(self.n_a)
        at = lax.rem(a + self.n_a - d, self.n_a)
        src = self.own if d == 0 else self.at(0, at)
        return remote(src, self.at(1, at), self.x, d, x_peer(self.n_a))

    def mine(self):
        a, _, _ = coords(self.n_a)
        return pltpu.make_async_copy(self.own, self.at(0, a), self.local)

    def start(self):
        self.x_copy(0).start()
        for d in range(1, self.n_a):
            self.z_copy(d).start()
        self.mine().start()

    def forward(self):
        for d in range(1, self.n_a):
            self.z_copy(d).wait_recv()
            self.x_copy(d).start()

    def finish(self):
        for d in range(1, self.n_a):
            self.z_copy(d).wait_send()
        for d in range(self.n_a):
            self.x_copy(d).wait()
        self.mine().wait()

    @staticmethod
    def scratch(n_a):
        return [DMA((n_a,)), DMA((n_a,)), DMA((n_a,)), DMA((n_a,)), DMA(())]


class TpGather:
    def __init__(self, n_a, own, out, sems):
        self.to_y = remote(own, out.at[:, 1], sems[:2], 0, y_peer(n_a))
        self.to_c = remote(own, out.at[:, 2], sems[:2], 1, c_peer(n_a))
        self.fwd = remote(out.at[:, 1], out.at[:, 3], sems[:2], 2, c_peer(n_a))
        self.mine = pltpu.make_async_copy(own, out.at[:, 0], sems[2])

    def start(self):
        self.to_y.start()
        self.to_c.start()
        self.mine.start()

    def forward(self):
        self.to_y.wait_recv()
        self.fwd.start()

    def finish(self):
        self.to_y.wait_send()
        self.to_c.wait()
        self.fwd.wait()
        self.mine.wait()

    @staticmethod
    def scratch():
        return [DMA((3,)), DMA((3,)), DMA(())]


class PlaneGather:
    def __init__(self, n_a, own, out, sems):
        half = own.shape[0] // 2
        h = [pl.ds(0, half), pl.ds(half, half)]
        x, y, c = x_peer(n_a), y_peer(n_a), c_peer(n_a)
        pair = sems[:2]

        def to(src, slot, i, peer, part=None):
            dst = out.at[slot] if part is None else out.at[slot, h[part]]
            return remote(src, dst, pair, i, peer)

        self.x0 = to(own.at[h[0]], 4, 0, x, 0)
        self.x1 = to(own.at[h[1]], 4, 1, x, 1)
        self.y0 = to(own.at[h[0]], 2, 2, y, 0)
        self.y1 = to(own.at[h[1]], 2, 3, y, 1)
        self.xd = to(out.at[2, h[0]], 6, 4, x, 0)
        self.yd = to(out.at[4, h[1]], 6, 5, y, 1)
        self.c = [to(own, 1, 6, c)] + [to(out.at[k], k + 1, 6 + k // 2, c) for k in (2, 4, 6)]
        self.mine = pltpu.make_async_copy(own, out.at[0], sems[2])

    def start(self):
        for copy in (self.x1, self.y0, self.x0, self.y1, self.c[0], self.mine):
            copy.start()

    def forward(self):
        self.y0.wait_recv()
        self.xd.start()
        self.x1.wait_recv()
        self.yd.start()
        self.y1.wait_recv()
        self.c[1].start()
        self.x0.wait_recv()
        self.c[2].start()
        self.xd.wait_recv()
        self.yd.wait_recv()
        self.c[3].start()

    def finish(self):
        for copy in (self.x0, self.x1, self.y0, self.y1, self.xd, self.yd):
            copy.wait_send()
        for copy in self.c:
            copy.wait()
        self.mine.wait()

    @staticmethod
    def scratch():
        return [DMA((10,)), DMA((10,)), DMA(())]


def comm_call(kernel, name, cid, out_shape, n_in, out_specs, scratch):
    return pl.pallas_call(
        kernel,
        name=name,
        out_shape=out_shape,
        in_specs=[VMEM_SPEC] * n_in,
        out_specs=out_specs,
        scratch_shapes=scratch,
        compiler_params=pltpu.CompilerParams(
            collective_id=cid, has_side_effects=True, vmem_limit_bytes=48 << 20
        ),
        cost_estimate=pl.CostEstimate(flops=0, bytes_accessed=64 << 20, transcendentals=0),
    )


def prologue_kernel(n_a, w_ref, x_ref, g_ref, m_ref, wall_ref, xall_ref, gall_ref, mgot_ref, *sems):
    a, b, tp = coords(n_a)
    n_dev = n_a * 8
    me = (a * 2 + b) * 4 + tp
    barrier = pltpu.get_barrier_semaphore()
    gather = FsdpGather(n_a, w_ref, wall_ref, lambda e, at: (at, b), sems[:5])
    rows = TpGather(n_a, x_ref, xall_ref, sems[5:8])
    g_sems = sems[8:10]
    swap = remote(m_ref, mgot_ref, sems[10:12], 0, x_peer(n_a))

    def peer(k):
        p = lax.rem(me + k, n_dev)
        return p // 4, p % 4

    @pl.loop(1, n_dev)
    def _(k):
        pl.semaphore_signal(barrier, inc=1, device_id=peer(k), device_id_type=MESH_ID)

    pl.semaphore_wait(barrier, n_dev - 1)

    def gain_copy(k):
        return remote(g_ref, gall_ref.at[me], g_sems, k, peer(k))

    @pl.loop(1, n_dev)
    def _(k):
        gain_copy(k).start()

    gather.start()
    rows.start()
    swap.start()
    gall_ref[me] = g_ref[...]
    rows.forward()
    gather.forward()

    @pl.loop(1, n_dev)
    def _(k):
        gain_copy(k).wait()

    rows.finish()
    gather.finish()
    swap.wait()


def prologue(w, x, gains, mlp):
    n_a = lax.axis_size("fsdp") // 2
    n_dev = n_a * 8
    seqs, rows, width = x.shape
    return comm_call(
        functools.partial(prologue_kernel, n_a),
        "prologue",
        1,
        (
            jax.ShapeDtypeStruct((n_a, 2) + w.shape, w.dtype),
            jax.ShapeDtypeStruct((seqs, 4, rows, width), x.dtype),
            jax.ShapeDtypeStruct((n_dev,) + gains.shape, gains.dtype),
            jax.ShapeDtypeStruct(mlp.shape, mlp.dtype),
        ),
        4,
        (HBM_SPEC, HBM_SPEC, VMEM_SPEC, HBM_SPEC),
        FsdpGather.scratch(n_a)
        + TpGather.scratch()
        + [DMA((n_dev,)), DMA((n_dev,)), DMA((1,)), DMA((1,))],
    )(w, x, gains, mlp)


def kv_gather_kernel(n_a, own_ref, gm_ref, out_ref, gmall_ref, *sems):
    greet([x_peer(n_a), y_peer(n_a), c_peer(n_a)] + a_peers(n_a))
    gather = FsdpGather(n_a, own_ref, out_ref, lambda e, a: (e, a), sems[:5])
    plane = PlaneGather(n_a, gm_ref, gmall_ref, sems[5:8])
    gather.start()
    plane.start()
    gather.forward()
    plane.forward()
    gather.finish()
    plane.finish()


def kv_gather(own, gm):
    n_a = lax.axis_size("fsdp") // 2
    return comm_call(
        functools.partial(kv_gather_kernel, n_a),
        "kv_gather",
        2,
        (
            jax.ShapeDtypeStruct((2, n_a) + own.shape, own.dtype),
            jax.ShapeDtypeStruct((8,) + gm.shape, gm.dtype),
        ),
        2,
        (HBM_SPEC, HBM_SPEC),
        FsdpGather.scratch(n_a) + PlaneGather.scratch(),
    )(own, gm)


def plane_gather_kernel(n_a, own_ref, out_ref, *sems):
    greet([x_peer(n_a), y_peer(n_a), c_peer(n_a)])
    plane = PlaneGather(n_a, own_ref, out_ref, sems)
    plane.start()
    plane.forward()
    plane.finish()


def plane_gather(own):
    n_a = lax.axis_size("fsdp") // 2
    return comm_call(
        functools.partial(plane_gather_kernel, n_a),
        "plane_gather",
        5,
        jax.ShapeDtypeStruct((8,) + own.shape, own.dtype),
        1,
        HBM_SPEC,
        PlaneGather.scratch(),
    )(own)


def tp_gather_kernel(n_a, own_ref, out_ref, *sems):
    greet([y_peer(n_a), c_peer(n_a)])
    rows = TpGather(n_a, own_ref, out_ref, sems)
    rows.start()
    rows.forward()
    rows.finish()


def tp_gather(own):
    n_a = lax.axis_size("fsdp") // 2
    seqs, rows, width = own.shape
    return comm_call(
        functools.partial(tp_gather_kernel, n_a),
        "tp_gather",
        6,
        jax.ShapeDtypeStruct((seqs, 4, rows, width), own.dtype),
        1,
        HBM_SPEC,
        TpGather.scratch(),
    )(own)


def tp_scatter_kernel(n_a, part_ref, out_ref, got_c, mid, got_y, c_send, c_recv, y_send, y_recv):
    greet([y_peer(n_a), c_peer(n_a)])
    seqs = part_ref.shape[0]
    to_c = [
        remote(part_ref.at[s, pl.ds(2, 2)], got_c.at[s], (c_send, c_recv), s, c_peer(n_a))
        for s in range(seqs)
    ]
    to_y = [
        remote(mid.at[s], got_y.at[s], (y_send, y_recv), s, y_peer(n_a)) for s in range(seqs)
    ]
    for copy in to_c:
        copy.start()
    for s in range(seqs):
        to_c[s].wait_recv()
        mid[s] = (part_ref[s, 1].astype(F32) + got_c[s, 1].astype(F32)).astype(BF16)
        out_ref[s] = part_ref[s, 0].astype(F32) + got_c[s, 0].astype(F32)
        to_y[s].start()
    for s in range(seqs):
        to_y[s].wait_recv()
        out_ref[s] = out_ref[s] + got_y[s].astype(F32)
    for copy in to_c + to_y:
        copy.wait_send()


def tp_scatter(part, name, cid):
    n_a = lax.axis_size("fsdp") // 2
    seqs, _, rows, width = part.shape
    return comm_call(
        functools.partial(tp_scatter_kernel, n_a),
        name,
        cid,
        jax.ShapeDtypeStruct((seqs, rows, width), F32),
        1,
        VMEM_SPEC,
        [
            pltpu.VMEM((seqs, 2, rows, width), BF16),
            pltpu.VMEM((seqs, rows, width), BF16),
            pltpu.VMEM((seqs, rows, width), BF16),
        ]
        + [DMA((seqs,))] * 4,
    )(part)


def plane_scatter_kernel(n_a, part_ref, out_ref, got_c, mid, got_x, got_y, got_d, send, recv):
    rows = part_ref.shape[1]
    half = rows // 2
    h0, h1 = pl.ds(0, half), pl.ds(half, half)
    x, y, c = x_peer(n_a), y_peer(n_a), c_peer(n_a)
    greet([x, y, c])
    sems = (send, recv)
    to_c = [remote(part_ref.at[2 * k + 1], got_c.at[k], sems, k, c) for k in range(4)]
    xd = remote(mid.at[3, h0], got_d.at[h0], sems, 4, x)
    yd = remote(mid.at[3, h1], got_d.at[h1], sems, 5, y)
    x0 = remote(mid.at[2, h0], got_x.at[h0], sems, 6, x)
    x1 = remote(mid.at[2, h1], got_x.at[h1], sems, 7, x)
    y0 = remote(mid.at[1, h0], got_y.at[h0], sems, 8, y)
    y1 = remote(mid.at[1, h1], got_y.at[h1], sems, 9, y)
    for k in (3, 2, 1, 0):
        to_c[k].start()

    def fold(k):
        to_c[k].wait_recv()
        mid[k] = (part_ref[2 * k].astype(F32) + got_c[k].astype(F32)).astype(BF16)

    fold(3)
    xd.start()
    yd.start()
    fold(2)
    x0.start()
    fold(1)
    y1.start()
    to_c[0].wait_recv()
    out_ref[...] = part_ref[0].astype(F32) + got_c[0].astype(F32)
    xd.wait_recv()
    mid[1, h0] = (mid[1, h0].astype(F32) + got_d[h0].astype(F32)).astype(BF16)
    y0.start()
    yd.wait_recv()
    mid[2, h1] = (mid[2, h1].astype(F32) + got_d[h1].astype(F32)).astype(BF16)
    x1.start()
    x0.wait_recv()
    y1.wait_recv()
    y0.wait_recv()
    x1.wait_recv()
    out_ref[...] = out_ref[...] + got_x[...].astype(F32) + got_y[...].astype(F32)
    for copy in to_c + [xd, yd, x0, x1, y0, y1]:
        copy.wait_send()


def plane_scatter(part):
    n_a = lax.axis_size("fsdp") // 2
    _, rows, width = part.shape
    return comm_call(
        functools.partial(plane_scatter_kernel, n_a),
        "plane_scatter",
        7,
        jax.ShapeDtypeStruct((rows, width), F32),
        1,
        VMEM_SPEC,
        [
            pltpu.VMEM((4, rows, width), BF16),
            pltpu.VMEM((4, rows, width), BF16),
            pltpu.VMEM((rows, width), BF16),
            pltpu.VMEM((rows, width), BF16),
            pltpu.VMEM((rows, width), BF16),
            DMA((10,)),
            DMA((10,)),
        ],
    )(part)


def plane_scatter_lazy(part):
    _, rows, width = part.shape
    part = part.reshape(4, 2, rows, width)
    part = part[:, 0].astype(F32) + swap_tp(part[:, 1], 1).astype(F32)
    part = part[:2] + swap_b(part[2:].astype(BF16)).astype(F32)
    return part[0] + swap_tp(part[1].astype(BF16), 2).astype(F32)


def kv_scatter_kernel(n_a, part_ref, out_ref, got, send, recv):
    a, b, tp = coords(n_a)
    peers = [
        (e, d, lax.rem(a + d, n_a), lax.rem(b + e, 2))
        for d in range(n_a)
        for e in range(2)
        if (d, e) != (0, 0)
    ]
    greet([(pa * 2 + pb, tp) for _, _, pa, pb in peers])
    copies = [
        remote(
            part_ref.at[e, pa], got.at[2 * d + e - 1], (send, recv), 2 * d + e - 1,
            (pa * 2 + pb, tp),
        )
        for e, d, pa, pb in peers
    ]
    for copy in copies:
        copy.start()
    total = part_ref[0, a].astype(F32)
    for i, copy in enumerate(copies):
        copy.wait_recv()
        total = total + got[i].astype(F32)
    out_ref[...] = total
    for copy in copies:
        copy.wait_send()


def kv_scatter(part):
    n_a = part.shape[1]
    n = 2 * n_a - 1
    return comm_call(
        functools.partial(kv_scatter_kernel, n_a),
        "kv_scatter",
        3,
        jax.ShapeDtypeStruct(part.shape[2:], F32),
        1,
        VMEM_SPEC,
        [pltpu.VMEM((n,) + part.shape[2:], part.dtype), DMA((n,)), DMA((n,))],
    )(part)


def gain_kernel(n_a, part_ref, out_ref, got, send, recv):
    a, b, tp = coords(n_a)
    n_dev = n_a * 8
    me = (a * 2 + b) * 4 + tp
    barrier = pltpu.get_barrier_semaphore()

    def peer(k):
        return lax.rem(me + k, n_dev)

    @pl.loop(1, n_dev)
    def _(k):
        p = peer(k)
        pl.semaphore_signal(barrier, inc=1, device_id=(p // 4, p % 4), device_id_type=MESH_ID)

    pl.semaphore_wait(barrier, n_dev - 1)

    def copy(k):
        p = peer(k)
        return remote(part_ref.at[p], got.at[k], (send, recv), k, (p // 4, p % 4))

    @pl.loop(1, n_dev)
    def _(k):
        copy(k).start()

    got[0] = part_ref[me]

    @pl.loop(1, n_dev)
    def _(k):
        copy(k).wait()

    out_ref[...] = jnp.sum(got[...], axis=0)


def scatter_gains(part):
    n_a = lax.axis_size("fsdp") // 2
    n = part.shape[0]
    return comm_call(
        functools.partial(gain_kernel, n_a),
        "gain_scatter",
        4,
        jax.ShapeDtypeStruct(part.shape[1:], F32),
        1,
        VMEM_SPEC,
        [pltpu.VMEM(part.shape, F32), DMA((n,)), DMA((n,))],
    )(part)


def row_offsets(idx, rows, y, c):
    ec = idx // (2 * rows)
    ey = (idx // rows) % 2
    return ((ey ^ y) * 2 + (ec ^ c)) * rows + idx % rows


def fill_bias(bias_ref, tab_ref, s, n_blocks, block, rows):
    y = tab_ref[s, n_blocks + 2]
    c = tab_ref[s, n_blocks + 3]
    prefix = tab_ref[s, n_blocks + 1]
    koff = row_offsets(lax.broadcasted_iota(jnp.int32, (block, block), 0), rows, y, c)
    qoff = row_offsets(lax.broadcasted_iota(jnp.int32, (block, block), 1), rows, y, c)
    qpos = qoff + tab_ref[s, n_blocks] * block
    for kb in range(n_blocks):
        kpos = koff + tab_ref[s, kb] * block
        ok = (kpos <= qpos) | (kpos < prefix)
        bias_ref[kb * block : (kb + 1) * block, :] = jnp.where(ok, 0.0, NEG)


def fwd_kernel(n_blocks, block, rows, step, tab_ref, q_ref, kv_ref, vt_ref, o_ref, lse_ref, bias_ref):
    s = pl.program_id(0)

    @pl.when(pl.program_id(1) == 0)
    def _():
        fill_bias(bias_ref, tab_ref, s, n_blocks, block, rows)

    q = q_ref[...]
    qz = jnp.concatenate([q, jnp.zeros_like(q)], axis=0)
    seq = n_blocks * block
    m = jnp.full((1, block), -jnp.inf, F32)
    l = jnp.zeros((1, block), F32)
    acc = jnp.zeros((HD, block), F32)
    for k0 in range(0, seq, step):
        sc = dot(kv_ref[k0 : k0 + step, :], qz, 1, 0) + bias_ref[k0 : k0 + step, :]
        m_new = jnp.maximum(m, jnp.max(sc, axis=0, keepdims=True))
        alpha = jnp.exp(m - m_new)
        p = jnp.exp(sc - m_new)
        l = l * alpha + jnp.sum(p, axis=0, keepdims=True)
        acc = acc * alpha + dot(vt_ref[:, k0 : k0 + step], p.astype(BF16), 1, 0)
        m = m_new
    o_ref[...] = (acc / l).astype(BF16)
    lse_ref[0] = m + jnp.log(l)


def bwd_kernel(
    n_blocks, block, rows, step, tab_ref, q_ref, kv_ref, kt_ref, go_ref, o_ref, lse_ref,
    dq_ref, dkv_ref, bias_ref, dkv_acc,
):
    s = pl.program_id(0)
    h = pl.program_id(1)

    @pl.when(h == 0)
    def _():
        fill_bias(bias_ref, tab_ref, s, n_blocks, block, rows)
        dkv_acc[...] = jnp.zeros_like(dkv_acc)

    q = q_ref[...]
    go = go_ref[...]
    zero = jnp.zeros_like(q)
    qz = jnp.concatenate([q, zero], axis=0)
    gz = jnp.concatenate([zero, go], axis=0)
    lse = lse_ref[0]
    delta = jnp.sum(go.astype(F32) * o_ref[...].astype(F32), axis=0, keepdims=True)
    seq = n_blocks * block
    dq = jnp.zeros((HD, block), F32)
    for k0 in range(0, seq, step):
        ks = slice(k0, k0 + step)
        kv = kv_ref[ks, :]
        p = jnp.exp(dot(kv, qz, 1, 0) + bias_ref[ks, :] - lse)
        ds = (p * (dot(kv, gz, 1, 0) - delta)).astype(BF16)
        dkv_acc[HD:, ks] += dot(go, p.astype(BF16), 1, 1)
        dkv_acc[:HD, ks] += dot(q, ds, 1, 1)
        dq = dq + dot(kt_ref[:, ks], ds, 1, 0)
    dq_ref[...] = dq

    @pl.when(h == pl.num_programs(1) - 1)
    def _():
        dkv_ref[...] = dkv_acc[...].T.astype(BF16)


def attention_specs(n_blocks, block):
    seq = n_blocks * block
    q_spec = pl.BlockSpec((HD, block), lambda s, h, t: (h, s))
    kv_spec = pl.BlockSpec((seq, 2 * HD), lambda s, h, t: (0, s))
    lse_spec = pl.BlockSpec((1, 1, block), lambda s, h, t: (h, 0, s))

    def half_spec(which):
        return pl.BlockSpec((HD, seq), lambda s, h, t: (2 * s + which, 0))

    return q_spec, kv_spec, lse_spec, half_spec


def attention_forward(tab, q_t, kv, kv_t, n_blocks, block, rows):
    heads, seqs, seq = q_t.shape[0] // HD, q_t.shape[1] // block, n_blocks * block
    q_spec, kv_spec, lse_spec, half_spec = attention_specs(n_blocks, block)
    return pl.pallas_call(
        functools.partial(fwd_kernel, n_blocks, block, rows, min(512, seq)),
        name="attn_fwd",
        out_shape=(
            jax.ShapeDtypeStruct(q_t.shape, BF16),
            jax.ShapeDtypeStruct((heads, 1, seqs * block), F32),
        ),
        grid_spec=pltpu.PrefetchScalarGridSpec(
            num_scalar_prefetch=1,
            grid=(seqs, heads),
            in_specs=[q_spec, kv_spec, half_spec(1)],
            out_specs=[q_spec, lse_spec],
            scratch_shapes=[pltpu.VMEM((seq, block), F32)],
        ),
        compiler_params=pltpu.CompilerParams(
            dimension_semantics=("arbitrary", "arbitrary"), vmem_limit_bytes=48 << 20
        ),
        cost_estimate=pl.CostEstimate(
            flops=16 * heads * seqs * block * seq * HD,
            bytes_accessed=4 * seqs * seq * 2 * HD,
            transcendentals=heads * seqs * block * seq,
        ),
    )(tab, q_t, kv, kv_t)


def attention_backward(tab, q_t, kv, kv_t, go_t, o_t, lse, n_blocks, block, rows):
    heads, seqs, seq = q_t.shape[0] // HD, q_t.shape[1] // block, n_blocks * block
    q_spec, kv_spec, lse_spec, half_spec = attention_specs(n_blocks, block)
    return pl.pallas_call(
        functools.partial(bwd_kernel, n_blocks, block, rows, min(512, seq)),
        name="attn_bwd",
        out_shape=(
            jax.ShapeDtypeStruct(q_t.shape, F32),
            jax.ShapeDtypeStruct((seq, seqs * 2 * HD), BF16),
        ),
        grid_spec=pltpu.PrefetchScalarGridSpec(
            num_scalar_prefetch=1,
            grid=(seqs, heads),
            in_specs=[q_spec, kv_spec, half_spec(0), q_spec, q_spec, lse_spec],
            out_specs=[q_spec, kv_spec],
            scratch_shapes=[pltpu.VMEM((seq, block), F32), pltpu.VMEM((2 * HD, seq), F32)],
        ),
        compiler_params=pltpu.CompilerParams(
            dimension_semantics=("arbitrary", "arbitrary"), vmem_limit_bytes=48 << 20
        ),
        cost_estimate=pl.CostEstimate(
            flops=40 * heads * seqs * block * seq * HD,
            bytes_accessed=8 * seqs * seq * 2 * HD,
            transcendentals=heads * seqs * block * seq,
        ),
    )(tab, q_t, kv, kv_t, go_t, o_t, lse)


def on_device(
    hidden_in, cotangent, gain_attn, w_query, w_key, w_value, w_out, gain_mlp, w_gate, w_up,
    w_down, prefix, block_order,
):
    seqs, rows, width = hidden_in.shape
    n_tp = lax.axis_size("tp")
    n_fsdp = lax.axis_size("fsdp")
    if n_tp != 4 or n_fsdp % 2 or w_key.shape[1] != HD:
        raise ValueError("unsupported mesh")
    n_a = n_fsdp // 2
    block = rows * n_tp
    tokens = seqs * block
    own = seqs * rows
    chunk = width // n_fsdp
    q_width = w_query.shape[1]
    ff = w_gate.shape[1] // 2
    fsdp_index = lax.axis_index("fsdp")
    b_idx = fsdp_index % 2
    tp_index = lax.axis_index("tp")
    y_idx, c_idx = tp_index // 2, tp_index % 2
    first = b_idx == 0

    def order(mine, other, axis):
        return jnp.concatenate(
            [jnp.where(first, mine, other), jnp.where(first, other, mine)], axis=axis
        )

    own_block = jnp.sum(
        jnp.where(jnp.arange(n_fsdp)[None, :] == fsdp_index, block_order, 0), axis=1
    )
    by_b = block_order.reshape(seqs, n_a, 2)
    even, odd = by_b[:, :, 0], by_b[:, :, 1]
    key_blocks = jnp.concatenate(
        [jnp.where(first, even, odd), jnp.where(first, odd, even)], axis=1
    )
    tab = jnp.concatenate(
        [
            key_blocks,
            own_block[:, None],
            prefix[:, None],
            jnp.broadcast_to(y_idx, (seqs, 1)),
            jnp.broadcast_to(c_idx, (seqs, 1)),
        ],
        axis=1,
    ).astype(jnp.int32)
    lane = jnp.arange(block, dtype=jnp.int32)
    offs = row_offsets(lane, rows, y_idx, c_idx)
    pos = (own_block[:, None] * block + offs[None, :]).reshape(tokens)
    frequency = THETA ** (-(jnp.arange(HD // 2, dtype=F32) * 2.0 / HD))
    angles = frequency[:, None] * pos.astype(F32)[None, :]
    cos_t = jnp.cos(angles)[None]
    sin_t = jnp.sin(angles)[None]

    def rotate_t(v):
        v = v.reshape(-1, HD, tokens)
        u1, u2 = v[:, : HD // 2], v[:, HD // 2 :]
        return jnp.concatenate(
            [u1 * cos_t - u2 * sin_t, u2 * cos_t + u1 * sin_t], axis=1
        ).reshape(-1, tokens)

    def rotate_back_t(v):
        v = v.reshape(-1, HD, tokens)
        u1, u2 = v[:, : HD // 2], v[:, HD // 2 :]
        return jnp.concatenate(
            [u1 * cos_t + u2 * sin_t, u2 * cos_t - u1 * sin_t], axis=1
        ).reshape(-1, tokens)

    piece = gain_attn.shape[0]
    fill = -2 * piece % 128
    gain_row = jnp.pad(jnp.concatenate([gain_attn, gain_mlp]), (0, fill))
    gain_row = jnp.broadcast_to(gain_row[None], (8, 2 * piece + fill))
    mlp_w = jnp.stack([w_gate, w_up, w_down.T])
    mlp_lo, mlp_hi = mlp_w[..., :ff], mlp_w[..., ff:]
    out_own = gather_a(w_out.T)
    qkv_w, x_all, gains, mlp_got = prologue(
        jnp.concatenate([w_query, w_key, w_value], axis=1),
        hidden_in,
        gain_row,
        jnp.where(first, mlp_hi, mlp_lo),
    )
    out_other = swap_b(out_own)
    out_w = order(
        out_own.reshape(n_a, 1, chunk, -1), out_other.reshape(n_a, 1, chunk, -1), 1
    ).reshape(width, -1)
    mlp_pair = order(jnp.where(first, mlp_lo, mlp_hi), mlp_got, 1)
    gate_w = gather_a(mlp_pair[0])
    up_w = gather_a(mlp_pair[1])
    down_w = gather_a(mlp_pair[2])
    gains = gains[:, 0]
    gain_first = gains[:, :piece].reshape(width)
    gain_second = gains[:, piece : 2 * piece].reshape(width)
    qkv_w = qkv_w.reshape(width, -1)
    cot = cotangent.reshape(own, width)

    x_all = x_all.reshape(seqs * block, width).astype(F32)
    h_first = (x_all * inverse_rms(x_all) * gain_first).astype(BF16)
    qkv_t = dot(qkv_w, h_first, 0, 1)
    q_t = (rotate_t(qkv_t[:q_width]).astype(BF16) * (HD**-0.5)).astype(BF16)
    kv_t = jnp.concatenate(
        [rotate_t(qkv_t[q_width : q_width + HD]), qkv_t[q_width + HD :]], axis=0
    ).astype(BF16)
    kv_own = (
        kv_t.reshape(2 * HD, seqs, block).transpose(2, 1, 0).reshape(block, seqs * 2 * HD)
    )
    kv, gm = kv_gather(kv_own, cot.astype(BF16))
    kv = kv.reshape(n_fsdp * block, -1)
    gm = gm.reshape(8 * own, width)
    kv_all_t = kv.T
    o_t, lse = attention_forward(tab, q_t, kv, kv_all_t, n_fsdp, block, rows)

    x_own = hidden_in.astype(F32).reshape(own, width)
    rms_first = inverse_rms(x_own)
    part = dot(o_t, out_w, 0, 1).astype(BF16).reshape(seqs, 4, rows, width)
    middle = x_own + tp_scatter(part, "out_scatter", 8).reshape(own, width)
    rms_second = inverse_rms(middle)
    h_second = plane_gather((middle * rms_second * gain_second).astype(BF16)).reshape(
        8 * own, width
    )

    gate = dot(h_second, gate_w, 1, 0)
    up = dot(h_second, up_w, 1, 0)
    sig = jax.nn.sigmoid(gate)
    hidden = (gate * sig * up).astype(BF16)
    down_g = scatter_a(dot(gm, hidden, 0, 0).astype(BF16))
    g_hidden = dot(gm, down_w, 1, 0)
    g_gate = (g_hidden * up * sig * (1.0 + gate * (1.0 - sig))).astype(BF16)
    g_up = (g_hidden * gate * sig).astype(BF16)
    g_h2 = (dot(g_gate, gate_w, 1, 1) + dot(g_up, up_w, 1, 1)).astype(BF16)
    g_h2 = plane_scatter(g_h2.reshape(8, own, width))
    gate_g = scatter_a(dot(h_second, g_gate, 0, 0).astype(BF16))
    up_g = scatter_a(dot(h_second, g_up, 0, 0).astype(BF16))
    layer_out = middle + plane_scatter_lazy(
        dot(hidden, down_w, 1, 1).astype(BF16).reshape(8, own, width)
    )
    g_mid_norm, gain_second_sum = norm_back(g_h2, middle, gain_second, rms_second)
    g_mid = cot + g_mid_norm

    ga = tp_gather(g_mid.astype(BF16).reshape(seqs, rows, width)).reshape(tokens, width)
    go_t = dot(out_w, ga, 0, 1).astype(BF16)
    dq_t, dkv = attention_backward(
        tab, q_t, kv, kv_all_t, go_t, o_t, lse, n_fsdp, block, rows
    )
    out_g = scatter_a(dot(ga, o_t, 0, 1).astype(BF16))
    dkv_own = kv_scatter(dkv.reshape(2, n_a, block, -1))
    dkv_t = dkv_own.reshape(block, seqs, 2 * HD).transpose(2, 1, 0).reshape(2 * HD, tokens)
    gq_t = rotate_back_t(dq_t * (HD**-0.5)).astype(BF16)
    gk_t = rotate_back_t(dkv_t[:HD]).astype(BF16)
    g_qkv_t = jnp.concatenate([gq_t, gk_t, dkv_t[HD:].astype(BF16)], axis=0)
    qkv_g = scatter_a(dot(h_first, g_qkv_t, 0, 1).astype(BF16))
    part = dot(g_qkv_t, qkv_w, 0, 1).astype(BF16).reshape(seqs, 4, rows, width)
    g_h1 = tp_scatter(part, "in_scatter", 9).reshape(own, width)
    g_in_norm, gain_first_sum = norm_back(g_h1, x_own, gain_first, rms_first)
    g_in = g_mid + g_in_norm
    gain_parts = jnp.concatenate(
        [
            gain_first_sum.reshape(-1, piece),
            gain_second_sum.reshape(-1, piece),
        ],
        axis=1,
    )
    gain_parts = jnp.pad(gain_parts, ((0, 0), (0, fill)))
    gain_parts = jnp.broadcast_to(
        gain_parts[:, None], (n_fsdp * 4, 8, 2 * piece + fill)
    )
    gain_sums = scatter_gains(gain_parts)[0]

    def split(part):
        lo, hi = part[..., :chunk, :], part[..., chunk:, :]
        return jnp.where(first, lo, hi), swap_b(jnp.where(first, hi, lo))

    def settle(part):
        mine, got = split(part)
        return mine.astype(F32) + got.astype(F32)

    out_g = settle(out_g)
    qkv_g = settle(qkv_g)
    mlp_g = order(*split(jnp.stack([gate_g, up_g, down_g])), 2).astype(F32)
    return (
        layer_out.reshape(hidden_in.shape),
        g_in.reshape(hidden_in.shape),
        gain_sums[:piece],
        qkv_g[:, :q_width],
        qkv_g[:, q_width : q_width + HD],
        qkv_g[:, q_width + HD :],
        out_g.T,
        gain_sums[piece : 2 * piece],
        mlp_g[0],
        mlp_g[1],
        mlp_g[2].T,
    )


def solution(mesh):
    rows = P(None, ("fsdp", "tp"), None)
    gain = P(("fsdp", "tp"))
    col = P("fsdp", "tp")
    row = P("tp", "fsdp")
    return jax.shard_map(
        on_device,
        mesh=mesh,
        in_specs=(rows, rows, gain, col, col, col, row, gain, col, col, row, P(), P()),
        out_specs=(rows, rows, gain, col, col, col, row, gain, col, col, row),
        check_vma=False,
    )
```
